32 devices in a mesh: grp: 4 (over z), sp: 8 (over y, x, core).
Axes of the slice: x: 2, y: 2, z: 4, core: 2. Of those that a mesh axis runs over, the one named last changes fastest.
Arguments:
- tokens: bfloat16 [2048, 2880], P(('grp', 'sp')), may hold values from -36 to 36
- query_weight: bfloat16 [2880, 2048], P(None, 'sp'), may hold values from -0.109375 to 0.109375
- key_value_weight: bfloat16 [2880, 1024], replicated, may hold values from -0.109375 to 0.109375
- block_places: int32 [16], replicated, may hold values from 0 to 15, each once
- sinks: float32 [32], replicated, may hold values from -1 to 5
Outputs:
- attended: bfloat16 [2048, 2048], P(('grp', 'sp'))
The draws below stay inside these ranges and needn't reach their ends.
Inputs may be any that keep to these rules, and one draw needn't show every extreme that they name: `block_places`: every sequence block appears once.
All inputs are finite; a program needn't handle non-finite values.
Results may differ from the reference program's by a relative error of at most 0.008.
The reference program's roundings to bfloat16 on the way count: a program that leaves them out, or rounds other values in their place, can miss the bound.
Values may be sent and summed in bfloat16 or wider, within the bound.
A program may use at most 128 MiB of HBM per device.

```python
import jax
import jax.numpy as jnp
from jax import lax

MODEL_WIDTH = 2880
QUERY_HEADS = 32
KEY_VALUE_HEADS = 8
HEAD_SIZE = 64
BLK = 128
NBLK = 16
SEQUENCE_TOKENS = 2048


def draw_tokens(key, part):
    base = jnp.clip(jax.random.normal(key, (SEQUENCE_TOKENS, MODEL_WIDTH), jnp.float32), -6.0, 6.0)
    return base.astype(jnp.bfloat16)


def block_levels(stream_key, extent, split, smallest, high):
    def one(position, shards_of):
        draws = jax.random.uniform(jax.random.fold_in(jax.random.fold_in(stream_key, 6), position), (shards_of,), jnp.float32, smallest / len(split), high / len(split))
        return jnp.repeat(jnp.exp(draws), extent[position] // shards_of).reshape((-1,) + (1,) * (len(extent) - position - 1))

    loudness = one(*split[0])
    for cut in split[1:]:
        loudness = loudness * one(*cut)
    return loudness


def scatter_about(stream_key, extent, width, most, cuts=(), kind=jnp.bfloat16):
    level = block_levels(stream_key, extent, cuts, -0.22, 0.18) if cuts else 1.0
    entries = jax.random.normal(stream_key, extent, jnp.float32) * width * level
    return jnp.minimum(jnp.maximum(entries, -most), most).astype(kind)


def setup_inputs(seed: int = 0) -> dict:
    keys = jax.random.split(jax.random.key(seed), 6)
    tokens = draw_tokens(jax.random.fold_in(keys[5], 71), 0)
    query_weight = scatter_about(keys[1], (MODEL_WIDTH, QUERY_HEADS * HEAD_SIZE), MODEL_WIDTH ** -0.5, 0.109375, ((1, 8),))
    key_value_weight = scatter_about(keys[2], (MODEL_WIDTH, 2 * KEY_VALUE_HEADS * HEAD_SIZE), MODEL_WIDTH ** -0.5, 0.109375)
    block_places = jax.random.permutation(keys[3], NBLK).astype(jnp.int32)
    sinks = jnp.clip(jax.random.uniform(keys[4], (QUERY_HEADS,), jnp.float32, -1.0, 5.0), -1.0, 5.0)
    return {"tokens": tokens, "query_weight": query_weight, "key_value_weight": key_value_weight, "block_places": block_places, "sinks": sinks}


rope_base = 150000.0
neg_large = -1.0e30


def rotate(vectors, angles):
    middle = vectors.shape[-1] // 2
    first_half = vectors[..., :middle]
    second_half = vectors[..., middle:]
    cosine = jnp.cos(angles)
    sine_part = jnp.sin(angles)
    return jnp.concatenate([first_half * cosine - second_half * sine_part, second_half * cosine + first_half * sine_part], axis=-1)


def reference(tokens, query_weight, key_value_weight, block_places, sinks):
    stored = jnp.arange(SEQUENCE_TOKENS, dtype=jnp.int32)
    blocks = stored // BLK
    places = block_places[blocks] * BLK + stored % BLK
    inverse = rope_base ** (-(jnp.arange(HEAD_SIZE // 2, dtype=jnp.float32) * 2.0) / HEAD_SIZE)
    angles = places.astype(jnp.float32)[:, None, None] * inverse[None, None, :]
    queries = jnp.dot(tokens, query_weight, preferred_element_type=jnp.float32).reshape(SEQUENCE_TOKENS, QUERY_HEADS, HEAD_SIZE)
    key_value_pair = jnp.dot(tokens, key_value_weight, preferred_element_type=jnp.float32)
    key_head_rows = key_value_pair[:, :KEY_VALUE_HEADS * HEAD_SIZE].reshape(SEQUENCE_TOKENS, KEY_VALUE_HEADS, HEAD_SIZE)
    value_head_rows = key_value_pair[:, KEY_VALUE_HEADS * HEAD_SIZE:].reshape(SEQUENCE_TOKENS, KEY_VALUE_HEADS, HEAD_SIZE).astype(jnp.bfloat16)
    queries = rotate(queries, angles).astype(jnp.bfloat16)
    key_head_rows = rotate(key_head_rows, angles).astype(jnp.bfloat16)
    query_sharing = QUERY_HEADS // KEY_VALUE_HEADS
    score_scale = HEAD_SIZE ** -0.5

    def single_head(head_number):
        head_keys = lax.dynamic_index_in_dim(key_head_rows, head_number, 1, keepdims=False).astype(jnp.float32)
        head_values = lax.dynamic_index_in_dim(value_head_rows, head_number, 1, keepdims=False).astype(jnp.float32)
        head_queries = lax.dynamic_slice_in_dim(queries, head_number * query_sharing, query_sharing, 1)
        head_sinks = lax.dynamic_slice_in_dim(sinks, head_number * query_sharing, query_sharing, 0)

        def one_block(query_block):
            first_row = query_block * BLK
            query_rows = lax.dynamic_slice_in_dim(head_queries, first_row, BLK, 0).astype(jnp.float32)
            row_places = lax.dynamic_slice_in_dim(places, first_row, BLK, 0)
            scores = jnp.einsum("qgd,kd->gqk", query_rows, head_keys) * score_scale
            allowed = places[None, :] <= row_places[:, None]
            scores = jnp.where(allowed[None], scores, neg_large)
            highest = jnp.maximum(jnp.max(scores, axis=-1, keepdims=True), head_sinks[:, None, None])
            weights = jnp.where(allowed[None], jnp.exp(scores - highest), 0.0)
            totals = jnp.sum(weights, axis=-1) + jnp.exp(head_sinks[:, None] - highest[..., 0])
            rounded = lax.optimization_barrier(weights.astype(jnp.bfloat16)).astype(jnp.float32)
            mixture = jnp.einsum("gqk,kd->qgd", rounded, head_values)
            return mixture / jnp.transpose(totals)[:, :, None]

        return lax.map(one_block, jnp.arange(SEQUENCE_TOKENS // BLK, dtype=jnp.int32))

    layer_output = lax.map(single_head, jnp.arange(KEY_VALUE_HEADS, dtype=jnp.int32))
    layer_output = jnp.transpose(layer_output, (1, 2, 0, 3, 4)).reshape(SEQUENCE_TOKENS, QUERY_HEADS * HEAD_SIZE)
    return layer_output.astype(jnp.bfloat16)
```

```python
import functools

import jax
import jax.numpy as jnp
from jax import lax
from jax.experimental import pallas as pl
from jax.experimental.pallas import tpu as pltpu
from jax.sharding import PartitionSpec as P

QUERY_HEADS = 32
HEAD_SIZE = 64
BPG = 4
LANES = 128

rope_base = 150000.0
neg_large = -1e30


def rotate_heads(x, cosine, sine):
    width = x.shape[1]
    half = HEAD_SIZE // 2
    if width % LANES:
        swapped = jnp.concatenate([x[:, half:], x[:, :half]], axis=1)
        return x * cosine[:, :width] + swapped * sine[:, :width]
    parts = []
    lane = lax.broadcasted_iota(jnp.int32, (x.shape[0], LANES), 1)
    first = lane % HEAD_SIZE < half
    for j in range(width // LANES):
        v = x[:, j * LANES : (j + 1) * LANES]
        swapped = jnp.where(first, pltpu.roll(v, LANES - half, 1), pltpu.roll(v, half, 1))
        parts.append(v * cosine + swapped * sine)
    return parts[0] if len(parts) == 1 else jnp.concatenate(parts, axis=1)


def kernel(
    grp, sp, qheads, kv_total,
    tok, wq_any, kvw_any, cos_ref, sin_ref, qpos, kpos, sink, out,
    toks, wq, wkv, kvb, q, abuf, obuf,
    wsem, tsend, tfwd, trecv, ksend, krecv, osend, orecv,
):
    s = lax.axis_index("sp")
    g = lax.axis_index("grp")
    rows = tok.shape[0]
    group_rows = rows * sp
    chips = sp // 2
    pair = 2 * rows
    qc = qheads * HEAD_SIZE
    c = s // 2
    par = s % 2
    partner = s + 1 - 2 * par
    head = s * kv_total // sp
    hpar = head % 2
    koff = pl.multiple_of(head // 2 * LANES, LANES)
    voff = pl.multiple_of(kv_total * HEAD_SIZE + head // 2 * LANES, LANES)

    wcopies = [
        pltpu.make_async_copy(wq_any, wq, wsem.at[0]),
        pltpu.make_async_copy(
            kvw_any.at[:, pl.ds(koff, LANES)], wkv.at[:, pl.ds(0, LANES)], wsem.at[1]
        ),
        pltpu.make_async_copy(
            kvw_any.at[:, pl.ds(voff, LANES)], wkv.at[:, pl.ds(LANES, LANES)], wsem.at[2]
        ),
    ]

    def send_tok(to):
        return pltpu.make_async_remote_copy(
            src_ref=tok, dst_ref=toks.at[s], send_sem=tsend.at[to], recv_sem=trecv.at[s],
            device_id={"sp": to},
        )

    def forward(slot):
        return pltpu.make_async_remote_copy(
            src_ref=toks.at[slot], dst_ref=toks.at[slot], send_sem=tfwd.at[slot],
            recv_sem=trecv.at[slot], device_id={"sp": partner},
        )

    def send_kv(chip, d):
        span = pl.ds(pl.multiple_of(g * group_rows + chip * pair, pair), pair)
        return pltpu.make_async_remote_copy(
            src_ref=kvb.at[span], dst_ref=kvb.at[span], send_sem=ksend.at[d, chip],
            recv_sem=krecv.at[g, chip], device_id={"grp": (g + d) % grp},
        )

    def recv_kv(chip, d):
        src = (g + d) % grp
        span = pl.ds(pl.multiple_of(src * group_rows + chip * pair, pair), pair)
        return pltpu.make_async_remote_copy(
            src_ref=kvb.at[span], dst_ref=kvb.at[span], send_sem=ksend.at[d, chip],
            recv_sem=krecv.at[src, chip], device_id={"grp": src},
        )

    def send_out(to):
        return pltpu.make_async_remote_copy(
            src_ref=abuf.at[to], dst_ref=obuf.at[s], send_sem=osend.at[to],
            recv_sem=orecv.at[s], device_id={"sp": to},
        )

    def recv_out(src):
        return pltpu.make_async_remote_copy(
            src_ref=abuf.at[src], dst_ref=obuf.at[src], send_sem=osend.at[src],
            recv_sem=orecv.at[src], device_id={"sp": src},
        )

    send_tok(partner).start()

    def start_tok(k, _):
        send_tok((c + k) % chips * 2 + par).start()
        return 0

    lax.fori_loop(1, chips, start_tok, 0)
    for copy in wcopies:
        copy.start()
    toks[s] = tok[...]
    for copy in wcopies:
        copy.wait()

    def project(k, _):
        chip = (c + chips - k) % chips

        @pl.when(k > 0)
        def _():
            slot = chip * 2 + par
            forward(slot).wait_recv()
            forward(slot).start()

        forward(chip * 2 + 1 - par).wait_recv()
        x = toks[pl.ds(chip * 2, 2)].reshape(pair, tok.shape[1])
        span = pl.ds(pl.multiple_of(chip * pair, pair), pair)
        cosine = cos_ref[span, :]
        sine = sin_ref[span, :]
        kv = jnp.dot(x, wkv[...], preferred_element_type=jnp.float32)
        keys = rotate_heads(kv[:, :LANES], cosine, sine)
        values = kv[:, LANES:]
        low = hpar == 0
        keys = jnp.where(low, keys, pltpu.roll(keys, HEAD_SIZE, 1))
        values = jnp.where(low, pltpu.roll(values, HEAD_SIZE, 1), values)
        lane = lax.broadcasted_iota(jnp.int32, (pair, LANES), 1)
        joined = jnp.where(lane < HEAD_SIZE, keys, values).astype(jnp.bfloat16)
        kvb[pl.ds(pl.multiple_of(g * group_rows + chip * pair, pair), pair), :] = joined
        for d in range(1, grp):
            send_kv(chip, d).start()
        qf = jnp.dot(x, wq[...], preferred_element_type=jnp.float32)
        qr = (rotate_heads(qf, cosine, sine) * HEAD_SIZE**-0.5).astype(jnp.bfloat16)
        zeros = jnp.zeros((pair, HEAD_SIZE), jnp.bfloat16)
        for h in range(qheads):
            q[h, span, :] = jnp.concatenate(
                [qr[:, h * HEAD_SIZE : (h + 1) * HEAD_SIZE], zeros], axis=1
            )
        return 0

    lax.fori_loop(0, chips, project, 0)

    def arrive(chip, _):
        for d in range(1, grp):
            recv_kv(chip, d).wait_recv()
        return 0

    lax.fori_loop(0, chips, arrive, 0)

    key_count = kvb.shape[0]
    chunk = min(key_count, 2048)
    chunks = key_count // chunk
    block = min(256, group_rows)
    tiles = block // rows

    def attention(b, _):
        span = pl.ds(pl.multiple_of(b * block, block), block)
        places = qpos[span, :]
        outs = []
        for h in range(qheads):
            qh = q[h, span, :]

            def visit(t, state):
                top, total, mix = state
                kspan = pl.ds(pl.multiple_of(t * chunk, chunk), chunk)
                kv = kvb[kspan, :]
                scores = lax.dot_general(
                    qh, kv, (((1,), (1,)), ((), ())), preferred_element_type=jnp.float32
                )
                allowed = kpos[:, kspan] <= places
                scores = jnp.where(allowed, scores, neg_large)
                higher = jnp.maximum(top, jnp.max(scores, axis=1, keepdims=True))
                weights = jnp.exp(scores - higher)
                factor = jnp.exp(top - higher)
                total = total * factor + jnp.sum(weights, axis=1, keepdims=True)
                mix = mix * factor + jnp.dot(
                    weights.astype(jnp.bfloat16), kv, preferred_element_type=jnp.float32
                )
                return higher, total, mix

            state = (
                jnp.full((block, 1), sink[s * qheads + h], jnp.float32),
                jnp.ones((block, 1), jnp.float32),
                jnp.zeros((block, LANES), jnp.float32),
            )
            if chunks == 1:
                state = visit(0, state)
            else:
                state = lax.fori_loop(0, chunks, visit, state)
            outs.append((state[2] / state[1])[:, HEAD_SIZE:])
        att = outs[0] if qheads == 1 else jnp.concatenate(outs, axis=1)
        abuf[pl.ds(b * tiles, tiles)] = att.astype(jnp.bfloat16).reshape(tiles, rows, qc)

        def ship(i, _):
            to = b * tiles + i

            @pl.when(to != s)
            def _():
                send_out(to).start()

            return 0

        lax.fori_loop(0, tiles, ship, 0)
        return 0

    lax.fori_loop(0, group_rows // block, attention, 0)
    obuf[s] = abuf[s]

    def drain(j, _):
        @pl.when(j != s)
        def _():
            recv_out(j).wait_recv()
            send_out(j).wait_send()

        return 0

    lax.fori_loop(0, sp, drain, 0)
    for j in range(sp):
        out[:, j * qc : (j + 1) * qc] = obuf[j]
    send_tok(partner).wait_send()

    def finish(k, _):
        send_tok((c + k) % chips * 2 + par).wait_send()
        forward((c + chips - k) % chips * 2 + par).wait_send()
        return 0

    lax.fori_loop(1, chips, finish, 0)

    def finish_kv(chip, _):
        for d in range(1, grp):
            send_kv(chip, d).wait_send()
        return 0

    lax.fori_loop(0, chips, finish_kv, 0)


def per_device(tokens, query_weight, key_value_weight, block_places, sinks):
    sp = lax.axis_size("sp")
    grp = lax.axis_size("grp")
    rows, width = tokens.shape
    group_rows = rows * sp
    block_rows = group_rows // BPG
    key_count = grp * group_rows
    qc = query_weight.shape[1]
    qheads = qc // HEAD_SIZE
    kv_total = key_value_weight.shape[1] // (2 * HEAD_SIZE)
    g = lax.axis_index("grp")

    within = jnp.arange(block_rows, dtype=jnp.int32)
    kpos = (block_places[:, None] * block_rows + within[None, :]).reshape(1, key_count)
    own = lax.dynamic_slice_in_dim(block_places, g * BPG, BPG, 0)
    qpos = (own[:, None] * block_rows + within[None, :]).reshape(group_rows, 1)
    freq = jnp.arange(HEAD_SIZE // 2, dtype=jnp.float32)
    inverse = rope_base ** (-(freq * 2.0) / HEAD_SIZE)
    lanes = jnp.tile(inverse, LANES // (HEAD_SIZE // 2))
    angles = qpos.astype(jnp.float32) * lanes[None, :]
    sign = jnp.where(jnp.arange(LANES) % HEAD_SIZE < HEAD_SIZE // 2, -1.0, 1.0)
    cosine = jnp.cos(angles)
    sine = jnp.sin(angles) * sign[None, :].astype(jnp.float32)

    vmem = pl.BlockSpec(memory_space=pltpu.VMEM)
    hbm = pl.BlockSpec(memory_space=pl.ANY)
    smem = pl.BlockSpec(memory_space=pltpu.SMEM)
    dma = pltpu.SemaphoreType.DMA
    return pl.pallas_call(
        functools.partial(kernel, grp, sp, qheads, kv_total),
        out_shape=jax.ShapeDtypeStruct((rows, qc * sp), jnp.bfloat16),
        in_specs=[vmem, hbm, hbm, vmem, vmem, vmem, vmem, smem],
        out_specs=vmem,
        scratch_shapes=[
            pltpu.VMEM((sp, rows, width), jnp.bfloat16),
            pltpu.VMEM((width, qc), jnp.bfloat16),
            pltpu.VMEM((width, 2 * LANES), jnp.bfloat16),
            pltpu.VMEM((key_count, LANES), jnp.bfloat16),
            pltpu.VMEM((qheads, group_rows, LANES), jnp.bfloat16),
            pltpu.VMEM((sp, rows, qc), jnp.bfloat16),
            pltpu.VMEM((sp, rows, qc), jnp.bfloat16),
            dma((3,)),
            dma((sp,)),
            dma((sp,)),
            dma((sp,)),
            dma((grp, sp // 2)),
            dma((grp, sp // 2)),
            dma((sp,)),
            dma((sp,)),
        ],
        compiler_params=pltpu.CompilerParams(
            has_side_effects=True, vmem_limit_bytes=60 * 1024 * 1024
        ),
    )(tokens, query_weight, key_value_weight, cosine, sine, qpos, kpos, sinks)


def solution(mesh):
    in_specs = (P(("grp", "sp"), None), P(None, "sp"), P(), P(), P())
    out_specs = P(("grp", "sp"), None)
    return jax.shard_map(
        per_device, mesh=mesh, in_specs=in_specs, out_specs=out_specs, check_vma=False
    )
```

```python
import functools

import jax
import jax.numpy as jnp
from jax import lax
from jax.experimental import pallas as pl
from jax.experimental.pallas import tpu as pltpu
from jax.sharding import PartitionSpec as P

QUERY_HEADS = 32
HEAD_SIZE = 64
BPG = 4
LANES = 128

rope_base = 150000.0
neg_large = -1e30


def rotate_heads(x, cosine, sine):
    width = x.shape[1]
    half = HEAD_SIZE // 2
    if width % LANES:
        swapped = jnp.concatenate([x[:, half:], x[:, :half]], axis=1)
        return x * cosine[:, :width] + swapped * sine[:, :width]
    parts = []
    lane = lax.broadcasted_iota(jnp.int32, (x.shape[0], LANES), 1)
    first = lane % HEAD_SIZE < half
    for j in range(width // LANES):
        v = x[:, j * LANES : (j + 1) * LANES]
        swapped = jnp.where(first, pltpu.roll(v, LANES - half, 1), pltpu.roll(v, half, 1))
        parts.append(v * cosine + swapped * sine)
    return parts[0] if len(parts) == 1 else jnp.concatenate(parts, axis=1)


def kernel(
    grp, sp, qheads, kv_total,
    tok, wq_any, kvw_any, inverse_ref, places_ref, sink, out,
    toks, wq, wkv, kvb, q, abuf, obuf, cos_ref, sin_ref, qpos, kpos,
    wsem, tsend, tfwd, trecv, ksend, krecv, osend, orecv,
):
    s = lax.axis_index("sp")
    g = lax.axis_index("grp")
    rows = tok.shape[0]
    group_rows = rows * sp
    chips = sp // 2
    pair = 2 * rows
    qc = qheads * HEAD_SIZE
    c = s // 2
    par = s % 2
    partner = s + 1 - 2 * par
    head = s * kv_total // sp
    hpar = head % 2
    koff = pl.multiple_of(head // 2 * LANES, LANES)
    voff = pl.multiple_of(kv_total * HEAD_SIZE + head // 2 * LANES, LANES)

    wcopies = [
        pltpu.make_async_copy(wq_any, wq, wsem.at[0]),
        pltpu.make_async_copy(
            kvw_any.at[:, pl.ds(koff, LANES)], wkv.at[:, pl.ds(0, LANES)], wsem.at[1]
        ),
        pltpu.make_async_copy(
            kvw_any.at[:, pl.ds(voff, LANES)], wkv.at[:, pl.ds(LANES, LANES)], wsem.at[2]
        ),
    ]

    def send_tok(to):
        return pltpu.make_async_remote_copy(
            src_ref=tok, dst_ref=toks.at[s], send_sem=tsend.at[to], recv_sem=trecv.at[s],
            device_id={"sp": to},
        )

    def forward(slot):
        return pltpu.make_async_remote_copy(
            src_ref=toks.at[slot], dst_ref=toks.at[slot], send_sem=tfwd.at[slot],
            recv_sem=trecv.at[slot], device_id={"sp": partner},
        )

    def send_kv(chip, d):
        span = pl.ds(pl.multiple_of(g * group_rows + chip * pair, pair), pair)
        return pltpu.make_async_remote_copy(
            src_ref=kvb.at[span], dst_ref=kvb.at[span], send_sem=ksend.at[d, chip],
            recv_sem=krecv.at[g, chip], device_id={"grp": (g + d) % grp},
        )

    def recv_kv(chip, d):
        src = (g + d) % grp
        span = pl.ds(pl.multiple_of(src * group_rows + chip * pair, pair), pair)
        return pltpu.make_async_remote_copy(
            src_ref=kvb.at[span], dst_ref=kvb.at[span], send_sem=ksend.at[d, chip],
            recv_sem=krecv.at[src, chip], device_id={"grp": src},
        )

    def send_out(to):
        return pltpu.make_async_remote_copy(
            src_ref=abuf.at[to], dst_ref=obuf.at[s], send_sem=osend.at[to],
            recv_sem=orecv.at[s], device_id={"sp": to},
        )

    def recv_out(src):
        return pltpu.make_async_remote_copy(
            src_ref=abuf.at[src], dst_ref=obuf.at[src], send_sem=osend.at[src],
            recv_sem=orecv.at[src], device_id={"sp": src},
        )

    send_tok(partner).start()

    def start_tok(k, _):
        send_tok((c + k) % chips * 2 + par).start()
        return 0

    lax.fori_loop(1, chips, start_tok, 0)
    for copy in wcopies:
        copy.start()
    toks[s] = tok[...]

    block_rows = group_rows // BPG
    for j in range(kpos.shape[1] // block_rows):
        within = lax.broadcasted_iota(jnp.int32, (1, block_rows), 1)
        kpos[:, j * block_rows : (j + 1) * block_rows] = places_ref[j] * block_rows + within
    wide = lax.broadcasted_iota(jnp.int32, (1, LANES), 1)
    half = HEAD_SIZE // 2
    inverse = inverse_ref[...]
    sign = jnp.where(wide % HEAD_SIZE < half, -1.0, 1.0)
    for j in range(BPG):
        rspan = slice(j * block_rows, (j + 1) * block_rows)
        within = lax.broadcasted_iota(jnp.int32, (block_rows, LANES), 0)
        place = places_ref[g * BPG + j] * block_rows + within
        qpos[rspan, :] = place[:, :1]
        angles = place.astype(jnp.float32) * inverse
        cos_ref[rspan, :] = jnp.cos(angles)
        sin_ref[rspan, :] = jnp.sin(angles) * sign
    for copy in wcopies:
        copy.wait()

    def project(k, _):
        chip = (c + chips - k) % chips

        @pl.when(k > 0)
        def _():
            slot = chip * 2 + par
            forward(slot).wait_recv()
            forward(slot).start()

        forward(chip * 2 + 1 - par).wait_recv()
        x = toks[pl.ds(chip * 2, 2)].reshape(pair, tok.shape[1])
        span = pl.ds(pl.multiple_of(chip * pair, pair), pair)
        cosine = cos_ref[span, :]
        sine = sin_ref[span, :]
        kv = jnp.dot(x, wkv[...], preferred_element_type=jnp.float32)
        keys = rotate_heads(kv[:, :LANES], cosine, sine)
        values = kv[:, LANES:]
        low = hpar == 0
        keys = jnp.where(low, keys, pltpu.roll(keys, HEAD_SIZE, 1))
        values = jnp.where(low, pltpu.roll(values, HEAD_SIZE, 1), values)
        lane = lax.broadcasted_iota(jnp.int32, (pair, LANES), 1)
        joined = jnp.where(lane < HEAD_SIZE, keys, values).astype(jnp.bfloat16)
        kvb[pl.ds(pl.multiple_of(g * group_rows + chip * pair, pair), pair), :] = joined
        for d in range(1, grp):
            send_kv(chip, d).start()
        qf = jnp.dot(x, wq[...], preferred_element_type=jnp.float32)
        qr = (rotate_heads(qf, cosine, sine) * HEAD_SIZE**-0.5).astype(jnp.bfloat16)
        zeros = jnp.zeros((pair, HEAD_SIZE), jnp.bfloat16)
        for h in range(qheads):
            q[h, span, :] = jnp.concatenate(
                [qr[:, h * HEAD_SIZE : (h + 1) * HEAD_SIZE], zeros], axis=1
            )
        return 0

    lax.fori_loop(0, chips, project, 0)

    def arrive(chip, _):
        for d in range(1, grp):
            recv_kv(chip, d).wait_recv()
        return 0

    lax.fori_loop(0, chips, arrive, 0)

    key_count = kvb.shape[0]
    chunk = min(key_count, 2048)
    chunks = key_count // chunk
    block = min(256, group_rows)
    tiles = block // rows

    def attention(b, _):
        span = pl.ds(pl.multiple_of(b * block, block), block)
        places = qpos[span, :]
        outs = []
        for h in range(qheads):
            qh = q[h, span, :]

            def visit(t, state):
                top, total, mix = state
                kspan = pl.ds(pl.multiple_of(t * chunk, chunk), chunk)
                kv = kvb[kspan, :]
                scores = lax.dot_general(
                    qh, kv, (((1,), (1,)), ((), ())), preferred_element_type=jnp.float32
                )
                allowed = kpos[:, kspan] <= places
                scores = jnp.where(allowed, scores, neg_large)
                higher = jnp.maximum(top, jnp.max(scores, axis=1, keepdims=True))
                weights = jnp.exp(scores - higher)
                factor = jnp.exp(top - higher)
                total = total * factor + jnp.sum(weights, axis=1, keepdims=True)
                mix = mix * factor + jnp.dot(
                    weights.astype(jnp.bfloat16), kv, preferred_element_type=jnp.float32
                )
                return higher, total, mix

            state = (
                jnp.full((block, 1), sink[s * qheads + h], jnp.float32),
                jnp.ones((block, 1), jnp.float32),
                jnp.zeros((block, LANES), jnp.float32),
            )
            if chunks == 1:
                state = visit(0, state)
            else:
                state = lax.fori_loop(0, chunks, visit, state)
            outs.append((state[2] / state[1])[:, HEAD_SIZE:])
        att = outs[0] if qheads == 1 else jnp.concatenate(outs, axis=1)
        abuf[pl.ds(b * tiles, tiles)] = att.astype(jnp.bfloat16).reshape(tiles, rows, qc)

        def ship(i, _):
            to = b * tiles + i

            @pl.when(to != s)
            def _():
                send_out(to).start()

            return 0

        lax.fori_loop(0, tiles, ship, 0)
        return 0

    lax.fori_loop(0, group_rows // block, attention, 0)
    obuf[s] = abuf[s]

    def drain(j, _):
        @pl.when(j != s)
        def _():
            recv_out(j).wait_recv()
            send_out(j).wait_send()

        return 0

    lax.fori_loop(0, sp, drain, 0)
    for j in range(sp):
        out[:, j * qc : (j + 1) * qc] = obuf[j]
    send_tok(partner).wait_send()

    def finish(k, _):
        send_tok((c + k) % chips * 2 + par).wait_send()
        forward((c + chips - k) % chips * 2 + par).wait_send()
        return 0

    lax.fori_loop(1, chips, finish, 0)

    def finish_kv(chip, _):
        for d in range(1, grp):
            send_kv(chip, d).wait_send()
        return 0

    lax.fori_loop(0, chips, finish_kv, 0)


def per_device(tokens, query_weight, key_value_weight, block_places, sinks):
    sp = lax.axis_size("sp")
    grp = lax.axis_size("grp")
    rows, width = tokens.shape
    group_rows = rows * sp
    key_count = grp * group_rows
    qc = query_weight.shape[1]
    qheads = qc // HEAD_SIZE
    kv_total = key_value_weight.shape[1] // (2 * HEAD_SIZE)
    freq = jnp.arange(HEAD_SIZE // 2, dtype=jnp.float32)
    inverse = rope_base ** (-(freq * 2.0) / HEAD_SIZE)
    inverse = jnp.tile(inverse, LANES // (HEAD_SIZE // 2)).reshape(1, LANES)

    vmem = pl.BlockSpec(memory_space=pltpu.VMEM)
    hbm = pl.BlockSpec(memory_space=pl.ANY)
    smem = pl.BlockSpec(memory_space=pltpu.SMEM)
    dma = pltpu.SemaphoreType.DMA
    return pl.pallas_call(
        functools.partial(kernel, grp, sp, qheads, kv_total),
        out_shape=jax.ShapeDtypeStruct((rows, qc * sp), jnp.bfloat16),
        in_specs=[vmem, hbm, hbm, vmem, smem, smem],
        out_specs=vmem,
        scratch_shapes=[
            pltpu.VMEM((sp, rows, width), jnp.bfloat16),
            pltpu.VMEM((width, qc), jnp.bfloat16),
            pltpu.VMEM((width, 2 * LANES), jnp.bfloat16),
            pltpu.VMEM((key_count, LANES), jnp.bfloat16),
            pltpu.VMEM((qheads, group_rows, LANES), jnp.bfloat16),
            pltpu.VMEM((sp, rows, qc), jnp.bfloat16),
            pltpu.VMEM((sp, rows, qc), jnp.bfloat16),
            pltpu.VMEM((group_rows, LANES), jnp.float32),
            pltpu.VMEM((group_rows, LANES), jnp.float32),
            pltpu.VMEM((group_rows, 1), jnp.int32),
            pltpu.VMEM((1, key_count), jnp.int32),
            dma((3,)),
            dma((sp,)),
            dma((sp,)),
            dma((sp,)),
            dma((grp, sp // 2)),
            dma((grp, sp // 2)),
            dma((sp,)),
            dma((sp,)),
        ],
        compiler_params=pltpu.CompilerParams(
            has_side_effects=True, vmem_limit_bytes=60 * 1024 * 1024
        ),
    )(tokens, query_weight, key_value_weight, inverse, block_places, sinks)


def solution(mesh):
    in_specs = (P(("grp", "sp"), None), P(None, "sp"), P(), P(), P())
    out_specs = P(("grp", "sp"), None)
    return jax.shard_map(
        per_device, mesh=mesh, in_specs=in_specs, out_specs=out_specs, check_vma=False
    )
```

```python
import functools

import jax
import jax.numpy as jnp
from jax import lax
from jax.experimental import pallas as pl
from jax.experimental.pallas import tpu as pltpu
from jax.sharding import PartitionSpec as P

QUERY_HEADS = 32
HEAD_SIZE = 64
BPG = 4
LANES = 128

rope_base = 150000.0
neg_large = -1e30


def rotate_heads(x, cosine, sine):
    width = x.shape[1]
    half = HEAD_SIZE // 2
    if width % LANES:
        swapped = jnp.concatenate([x[:, half:], x[:, :half]], axis=1)
        return x * cosine[:, :width] + swapped * sine[:, :width]
    parts = []
    lane = lax.broadcasted_iota(jnp.int32, (x.shape[0], LANES), 1)
    first = lane % HEAD_SIZE < half
    for j in range(width // LANES):
        v = x[:, j * LANES : (j + 1) * LANES]
        swapped = jnp.where(first, pltpu.roll(v, LANES - half, 1), pltpu.roll(v, half, 1))
        parts.append(v * cosine + swapped * sine)
    return parts[0] if len(parts) == 1 else jnp.concatenate(parts, axis=1)


def kernel(
    grp, sp, qheads, kv_total,
    tok, wq_any, kvw_any, inverse_ref, places_ref, sink, out,
    toks, wq, wkv, kvb, q, abuf, obuf, cos_ref, sin_ref, qpos, kpos,
    wsem, tsend, tfwd, trecv, ksend, krecv, osend, orecv,
):
    s = lax.axis_index("sp")
    g = lax.axis_index("grp")
    rows = tok.shape[0]
    group_rows = rows * sp
    chips = sp // 2
    pair = 2 * rows
    qc = qheads * HEAD_SIZE
    c = s // 2
    par = s % 2
    partner = s + 1 - 2 * par
    head = s * kv_total // sp
    hpar = head % 2
    koff = pl.multiple_of(head // 2 * LANES, LANES)
    voff = pl.multiple_of(kv_total * HEAD_SIZE + head // 2 * LANES, LANES)

    wcopies = [
        pltpu.make_async_copy(wq_any, wq, wsem.at[0]),
        pltpu.make_async_copy(
            kvw_any.at[:, pl.ds(koff, LANES)], wkv.at[:, pl.ds(0, LANES)], wsem.at[1]
        ),
        pltpu.make_async_copy(
            kvw_any.at[:, pl.ds(voff, LANES)], wkv.at[:, pl.ds(LANES, LANES)], wsem.at[2]
        ),
    ]

    def send_tok(to):
        return pltpu.make_async_remote_copy(
            src_ref=tok, dst_ref=toks.at[s], send_sem=tsend.at[to], recv_sem=trecv.at[s],
            device_id={"sp": to},
        )

    def forward(slot):
        return pltpu.make_async_remote_copy(
            src_ref=toks.at[slot], dst_ref=toks.at[slot], send_sem=tfwd.at[slot],
            recv_sem=trecv.at[slot], device_id={"sp": partner},
        )

    def send_kv(chip, d):
        span = pl.ds(pl.multiple_of(g * group_rows + chip * pair, pair), pair)
        return pltpu.make_async_remote_copy(
            src_ref=kvb.at[span], dst_ref=kvb.at[span], send_sem=ksend.at[d, chip],
            recv_sem=krecv.at[g, chip], device_id={"grp": (g + d) % grp},
        )

    def recv_kv(chip, d):
        src = (g + d) % grp
        span = pl.ds(pl.multiple_of(src * group_rows + chip * pair, pair), pair)
        return pltpu.make_async_remote_copy(
            src_ref=kvb.at[span], dst_ref=kvb.at[span], send_sem=ksend.at[d, chip],
            recv_sem=krecv.at[src, chip], device_id={"grp": src},
        )

    def send_out(to):
        return pltpu.make_async_remote_copy(
            src_ref=abuf.at[to], dst_ref=obuf.at[s], send_sem=osend.at[to],
            recv_sem=orecv.at[s], device_id={"sp": to},
        )

    def recv_out(src):
        return pltpu.make_async_remote_copy(
            src_ref=abuf.at[src], dst_ref=obuf.at[src], send_sem=osend.at[src],
            recv_sem=orecv.at[src], device_id={"sp": src},
        )

    send_tok(partner).start()

    def start_tok(k, _):
        send_tok((c + k) % chips * 2 + par).start()
        return 0

    lax.fori_loop(1, chips, start_tok, 0)
    for copy in wcopies:
        copy.start()
    toks[s] = tok[...]

    block_rows = group_rows // BPG
    for j in range(kpos.shape[1] // block_rows):
        within = lax.broadcasted_iota(jnp.int32, (1, block_rows), 1)
        kpos[:, j * block_rows : (j + 1) * block_rows] = places_ref[j] * block_rows + within
    wide = lax.broadcasted_iota(jnp.int32, (1, LANES), 1)
    half = HEAD_SIZE // 2
    inverse = inverse_ref[...]
    sign = jnp.where(wide % HEAD_SIZE < half, -1.0, 1.0)
    for j in range(BPG):
        rspan = slice(j * block_rows, (j + 1) * block_rows)
        within = lax.broadcasted_iota(jnp.int32, (block_rows, LANES), 0)
        place = places_ref[g * BPG + j] * block_rows + within
        qpos[rspan, :] = place[:, :1]
        angles = place.astype(jnp.float32) * inverse
        cos_ref[rspan, :] = jnp.cos(angles)
        sin_ref[rspan, :] = jnp.sin(angles) * sign
    for copy in wcopies:
        copy.wait()

    def project(k, _):
        chip = (c + chips - k) % chips

        @pl.when(k > 0)
        def _():
            slot = chip * 2 + par
            forward(slot).wait_recv()
            forward(slot).start()

        forward(chip * 2 + 1 - par).wait_recv()
        x = toks[pl.ds(chip * 2, 2)].reshape(pair, tok.shape[1])
        span = pl.ds(pl.multiple_of(chip * pair, pair), pair)
        cosine = cos_ref[span, :]
        sine = sin_ref[span, :]
        kv = jnp.dot(x, wkv[...], preferred_element_type=jnp.float32)
        keys = rotate_heads(kv[:, :LANES], cosine, sine)
        values = kv[:, LANES:]
        low = hpar == 0
        keys = jnp.where(low, keys, pltpu.roll(keys, HEAD_SIZE, 1))
        values = jnp.where(low, pltpu.roll(values, HEAD_SIZE, 1), values)
        lane = lax.broadcasted_iota(jnp.int32, (pair, LANES), 1)
        joined = jnp.where(lane < HEAD_SIZE, keys, values).astype(jnp.bfloat16)
        kvb[pl.ds(pl.multiple_of(g * group_rows + chip * pair, pair), pair), :] = joined
        for d in range(1, grp):
            send_kv(chip, d).start()
        qf = jnp.dot(x, wq[...], preferred_element_type=jnp.float32)
        qr = (rotate_heads(qf, cosine, sine) * HEAD_SIZE**-0.5).astype(jnp.bfloat16)
        zeros = jnp.zeros((pair, HEAD_SIZE), jnp.bfloat16)
        for h in range(qheads):
            q[h, span, :] = jnp.concatenate(
                [qr[:, h * HEAD_SIZE : (h + 1) * HEAD_SIZE], zeros], axis=1
            )
        return 0

    lax.fori_loop(0, chips, project, 0)

    def arrive(chip, _):
        for d in range(1, grp):
            recv_kv(chip, d).wait_recv()
        return 0

    lax.fori_loop(0, chips, arrive, 0)

    key_count = kvb.shape[0]
    chunk = min(key_count, 2048)
    chunks = key_count // chunk
    block = min(256, group_rows)
    tiles = block // rows

    blocks = group_rows // block

    def attention(turn, _):
        b = (s // tiles + 1 + turn) % blocks
        span = pl.ds(pl.multiple_of(b * block, block), block)
        places = qpos[span, :]
        outs = []
        for h in range(qheads):
            qh = q[h, span, :]

            def visit(t, state):
                top, total, mix = state
                kspan = pl.ds(pl.multiple_of(t * chunk, chunk), chunk)
                kv = kvb[kspan, :]
                scores = lax.dot_general(
                    qh, kv, (((1,), (1,)), ((), ())), preferred_element_type=jnp.float32
                )
                allowed = kpos[:, kspan] <= places
                scores = jnp.where(allowed, scores, neg_large)
                higher = jnp.maximum(top, jnp.max(scores, axis=1, keepdims=True))
                weights = jnp.exp(scores - higher)
                factor = jnp.exp(top - higher)
                total = total * factor + jnp.sum(weights, axis=1, keepdims=True)
                mix = mix * factor + jnp.dot(
                    weights.astype(jnp.bfloat16), kv, preferred_element_type=jnp.float32
                )
                return higher, total, mix

            state = (
                jnp.full((block, 1), sink[s * qheads + h], jnp.float32),
                jnp.ones((block, 1), jnp.float32),
                jnp.zeros((block, LANES), jnp.float32),
            )
            if chunks == 1:
                state = visit(0, state)
            else:
                state = lax.fori_loop(0, chunks, visit, state)
            outs.append((state[2] / state[1])[:, HEAD_SIZE:])
        att = outs[0] if qheads == 1 else jnp.concatenate(outs, axis=1)
        abuf[pl.ds(b * tiles, tiles)] = att.astype(jnp.bfloat16).reshape(tiles, rows, qc)

        def ship(i, _):
            to = b * tiles + i

            @pl.when(to != s)
            def _():
                send_out(to).start()

            return 0

        lax.fori_loop(0, tiles, ship, 0)
        return 0

    lax.fori_loop(0, blocks, attention, 0)
    obuf[s] = abuf[s]

    def drain(j, _):
        @pl.when(j != s)
        def _():
            recv_out(j).wait_recv()
            send_out(j).wait_send()

        return 0

    lax.fori_loop(0, sp, drain, 0)
    for j in range(sp):
        out[:, j * qc : (j + 1) * qc] = obuf[j]
    send_tok(partner).wait_send()

    def finish(k, _):
        send_tok((c + k) % chips * 2 + par).wait_send()
        forward((c + chips - k) % chips * 2 + par).wait_send()
        return 0

    lax.fori_loop(1, chips, finish, 0)

    def finish_kv(chip, _):
        for d in range(1, grp):
            send_kv(chip, d).wait_send()
        return 0

    lax.fori_loop(0, chips, finish_kv, 0)


def per_device(tokens, query_weight, key_value_weight, block_places, sinks):
    sp = lax.axis_size("sp")
    grp = lax.axis_size("grp")
    rows, width = tokens.shape
    group_rows = rows * sp
    key_count = grp * group_rows
    qc = query_weight.shape[1]
    qheads = qc // HEAD_SIZE
    kv_total = key_value_weight.shape[1] // (2 * HEAD_SIZE)
    freq = jnp.arange(HEAD_SIZE // 2, dtype=jnp.float32)
    inverse = rope_base ** (-(freq * 2.0) / HEAD_SIZE)
    inverse = jnp.tile(inverse, LANES // (HEAD_SIZE // 2)).reshape(1, LANES)

    vmem = pl.BlockSpec(memory_space=pltpu.VMEM)
    hbm = pl.BlockSpec(memory_space=pl.ANY)
    smem = pl.BlockSpec(memory_space=pltpu.SMEM)
    dma = pltpu.SemaphoreType.DMA
    return pl.pallas_call(
        functools.partial(kernel, grp, sp, qheads, kv_total),
        out_shape=jax.ShapeDtypeStruct((rows, qc * sp), jnp.bfloat16),
        in_specs=[vmem, hbm, hbm, vmem, smem, smem],
        out_specs=vmem,
        scratch_shapes=[
            pltpu.VMEM((sp, rows, width), jnp.bfloat16),
            pltpu.VMEM((width, qc), jnp.bfloat16),
            pltpu.VMEM((width, 2 * LANES), jnp.bfloat16),
            pltpu.VMEM((key_count, LANES), jnp.bfloat16),
            pltpu.VMEM((qheads, group_rows, LANES), jnp.bfloat16),
            pltpu.VMEM((sp, rows, qc), jnp.bfloat16),
            pltpu.VMEM((sp, rows, qc), jnp.bfloat16),
            pltpu.VMEM((group_rows, LANES), jnp.float32),
            pltpu.VMEM((group_rows, LANES), jnp.float32),
            pltpu.VMEM((group_rows, 1), jnp.int32),
            pltpu.VMEM((1, key_count), jnp.int32),
            dma((3,)),
            dma((sp,)),
            dma((sp,)),
            dma((sp,)),
            dma((grp, sp // 2)),
            dma((grp, sp // 2)),
            dma((sp,)),
            dma((sp,)),
        ],
        compiler_params=pltpu.CompilerParams(
            has_side_effects=True, vmem_limit_bytes=60 * 1024 * 1024
        ),
    )(tokens, query_weight, key_value_weight, inverse, block_places, sinks)


def solution(mesh):
    in_specs = (P(("grp", "sp"), None), P(None, "sp"), P(), P(), P())
    out_specs = P(("grp", "sp"), None)
    return jax.shard_map(
        per_device, mesh=mesh, in_specs=in_specs, out_specs=out_specs, check_vma=False
    )
```

```python
import functools

import jax
import jax.numpy as jnp
from jax import lax
from jax.experimental import pallas as pl
from jax.experimental.pallas import tpu as pltpu
from jax.sharding import PartitionSpec as P

QUERY_HEADS = 32
HEAD_SIZE = 64
BPG = 4
LANES = 128

rope_base = 150000.0
neg_large = -1e30


def rotate_heads(x, cosine, sine):
    width = x.shape[1]
    half = HEAD_SIZE // 2
    if width % LANES:
        swapped = jnp.concatenate([x[:, half:], x[:, :half]], axis=1)
        return x * cosine[:, :width] + swapped * sine[:, :width]
    parts = []
    lane = lax.broadcasted_iota(jnp.int32, (x.shape[0], LANES), 1)
    first = lane % HEAD_SIZE < half
    for j in range(width // LANES):
        v = x[:, j * LANES : (j + 1) * LANES]
        swapped = jnp.where(first, pltpu.roll(v, LANES - half, 1), pltpu.roll(v, half, 1))
        parts.append(v * cosine + swapped * sine)
    return parts[0] if len(parts) == 1 else jnp.concatenate(parts, axis=1)


def kernel(
    grp, sp, qheads, kv_total,
    tok, wq_any, kvw_any, inverse_ref, places_ref, sink, out,
    toks, wq, wkv, kvb, q, abuf, obuf, cos_ref, sin_ref, qpos, kpos,
    wsem, tsend, tfwd, trecv, ksend, krecv, osend, orecv,
):
    s = lax.axis_index("sp")
    g = lax.axis_index("grp")
    rows = tok.shape[0]
    group_rows = rows * sp
    chips = sp // 2
    pair = 2 * rows
    qc = qheads * HEAD_SIZE
    c = s // 2
    par = s % 2
    partner = s + 1 - 2 * par
    head = s * kv_total // sp
    hpar = head % 2
    koff = pl.multiple_of(head // 2 * LANES, LANES)
    voff = pl.multiple_of(kv_total * HEAD_SIZE + head // 2 * LANES, LANES)

    wcopies = [
        pltpu.make_async_copy(wq_any, wq, wsem.at[0]),
        pltpu.make_async_copy(
            kvw_any.at[:, pl.ds(koff, LANES)], wkv.at[:, pl.ds(0, LANES)], wsem.at[1]
        ),
        pltpu.make_async_copy(
            kvw_any.at[:, pl.ds(voff, LANES)], wkv.at[:, pl.ds(LANES, LANES)], wsem.at[2]
        ),
    ]

    def send_tok(to):
        return pltpu.make_async_remote_copy(
            src_ref=tok, dst_ref=toks.at[s], send_sem=tsend.at[to], recv_sem=trecv.at[s],
            device_id={"sp": to},
        )

    def forward(slot):
        return pltpu.make_async_remote_copy(
            src_ref=toks.at[slot], dst_ref=toks.at[slot], send_sem=tfwd.at[slot],
            recv_sem=trecv.at[slot], device_id={"sp": partner},
        )

    def send_kv(chip, d):
        span = pl.ds(pl.multiple_of(g * group_rows + chip * pair, pair), pair)
        return pltpu.make_async_remote_copy(
            src_ref=kvb.at[span], dst_ref=kvb.at[span], send_sem=ksend.at[d, chip],
            recv_sem=krecv.at[g, chip], device_id={"grp": (g + d) % grp},
        )

    def recv_kv(chip, d):
        src = (g + d) % grp
        span = pl.ds(pl.multiple_of(src * group_rows + chip * pair, pair), pair)
        return pltpu.make_async_remote_copy(
            src_ref=kvb.at[span], dst_ref=kvb.at[span], send_sem=ksend.at[d, chip],
            recv_sem=krecv.at[src, chip], device_id={"grp": src},
        )

    def send_out(to):
        return pltpu.make_async_remote_copy(
            src_ref=abuf.at[to], dst_ref=obuf.at[s], send_sem=osend.at[to],
            recv_sem=orecv.at[s], device_id={"sp": to},
        )

    def recv_out(src):
        return pltpu.make_async_remote_copy(
            src_ref=abuf.at[src], dst_ref=obuf.at[src], send_sem=osend.at[src],
            recv_sem=orecv.at[src], device_id={"sp": src},
        )

    send_tok(partner).start()

    def start_tok(k, _):
        send_tok((c + k) % chips * 2 + par).start()
        return 0

    lax.fori_loop(1, chips, start_tok, 0)
    for copy in wcopies:
        copy.start()
    toks[s] = tok[...]

    block_rows = group_rows // BPG
    for j in range(kpos.shape[1] // block_rows):
        within = lax.broadcasted_iota(jnp.int32, (1, block_rows), 1)
        kpos[:, j * block_rows : (j + 1) * block_rows] = places_ref[j] * block_rows + within
    wide = lax.broadcasted_iota(jnp.int32, (1, LANES), 1)
    half = HEAD_SIZE // 2
    inverse = inverse_ref[...]
    sign = jnp.where(wide % HEAD_SIZE < half, -1.0, 1.0)
    for j in range(BPG):
        rspan = slice(j * block_rows, (j + 1) * block_rows)
        within = lax.broadcasted_iota(jnp.int32, (block_rows, LANES), 0)
        place = places_ref[g * BPG + j] * block_rows + within
        qpos[rspan, :] = place[:, :1]
        angles = place.astype(jnp.float32) * inverse
        cos_ref[rspan, :] = jnp.cos(angles)
        sin_ref[rspan, :] = jnp.sin(angles) * sign
    for copy in wcopies:
        copy.wait()

    def project(k, _):
        chip = (c + chips - k) % chips

        def relay(turn):
            slot = (c + chips - turn) % chips * 2 + par
            forward(slot).wait_recv()
            forward(slot).start()

        @pl.when(k == 1)
        def _():
            relay(k)

        @pl.when(jnp.logical_and(k > 0, k + 1 < chips))
        def _():
            relay(k + 1)

        forward(chip * 2 + 1 - par).wait_recv()
        x = toks[pl.ds(chip * 2, 2)].reshape(pair, tok.shape[1])
        span = pl.ds(pl.multiple_of(chip * pair, pair), pair)
        cosine = cos_ref[span, :]
        sine = sin_ref[span, :]
        kv = jnp.dot(x, wkv[...], preferred_element_type=jnp.float32)
        keys = rotate_heads(kv[:, :LANES], cosine, sine)
        values = kv[:, LANES:]
        low = hpar == 0
        keys = jnp.where(low, keys, pltpu.roll(keys, HEAD_SIZE, 1))
        values = jnp.where(low, pltpu.roll(values, HEAD_SIZE, 1), values)
        lane = lax.broadcasted_iota(jnp.int32, (pair, LANES), 1)
        joined = jnp.where(lane < HEAD_SIZE, keys, values).astype(jnp.bfloat16)
        kvb[pl.ds(pl.multiple_of(g * group_rows + chip * pair, pair), pair), :] = joined
        for d in range(1, grp):
            send_kv(chip, d).start()
        qf = jnp.dot(x, wq[...], preferred_element_type=jnp.float32)
        qr = (rotate_heads(qf, cosine, sine) * HEAD_SIZE**-0.5).astype(jnp.bfloat16)
        zeros = jnp.zeros((pair, HEAD_SIZE), jnp.bfloat16)
        for h in range(qheads):
            q[h, span, :] = jnp.concatenate(
                [qr[:, h * HEAD_SIZE : (h + 1) * HEAD_SIZE], zeros], axis=1
            )
        return 0

    lax.fori_loop(0, chips, project, 0)

    def arrive(chip, _):
        for d in range(1, grp):
            recv_kv(chip, d).wait_recv()
        return 0

    lax.fori_loop(0, chips, arrive, 0)

    key_count = kvb.shape[0]
    chunk = min(key_count, 2048)
    chunks = key_count // chunk
    block = min(256, group_rows)
    tiles = block // rows

    blocks = group_rows // block

    def attention(turn, _):
        b = (s // tiles + 1 + turn) % blocks
        span = pl.ds(pl.multiple_of(b * block, block), block)
        places = qpos[span, :]
        outs = []
        for h in range(qheads):
            qh = q[h, span, :]

            def visit(t, state):
                top, total, mix = state
                kspan = pl.ds(pl.multiple_of(t * chunk, chunk), chunk)
                kv = kvb[kspan, :]
                scores = lax.dot_general(
                    qh, kv, (((1,), (1,)), ((), ())), preferred_element_type=jnp.float32
                )
                allowed = kpos[:, kspan] <= places
                scores = jnp.where(allowed, scores, neg_large)
                higher = jnp.maximum(top, jnp.max(scores, axis=1, keepdims=True))
                weights = jnp.exp(scores - higher)
                factor = jnp.exp(top - higher)
                total = total * factor + jnp.sum(weights, axis=1, keepdims=True)
                mix = mix * factor + jnp.dot(
                    weights.astype(jnp.bfloat16), kv, preferred_element_type=jnp.float32
                )
                return higher, total, mix

            state = (
                jnp.full((block, 1), sink[s * qheads + h], jnp.float32),
                jnp.ones((block, 1), jnp.float32),
                jnp.zeros((block, LANES), jnp.float32),
            )
            if chunks == 1:
                state = visit(0, state)
            else:
                state = lax.fori_loop(0, chunks, visit, state)
            outs.append((state[2] / state[1])[:, HEAD_SIZE:])
        att = outs[0] if qheads == 1 else jnp.concatenate(outs, axis=1)
        abuf[pl.ds(b * tiles, tiles)] = att.astype(jnp.bfloat16).reshape(tiles, rows, qc)

        def ship(i, _):
            to = b * tiles + i

            @pl.when(to != s)
            def _():
                send_out(to).start()

            return 0

        lax.fori_loop(0, tiles, ship, 0)
        return 0

    lax.fori_loop(0, blocks, attention, 0)
    obuf[s] = abuf[s]

    def drain(j, _):
        @pl.when(j != s)
        def _():
            recv_out(j).wait_recv()
            send_out(j).wait_send()

        return 0

    lax.fori_loop(0, sp, drain, 0)
    for j in range(sp):
        out[:, j * qc : (j + 1) * qc] = obuf[j]
    send_tok(partner).wait_send()

    def finish(k, _):
        send_tok((c + k) % chips * 2 + par).wait_send()
        forward((c + chips - k) % chips * 2 + par).wait_send()
        return 0

    lax.fori_loop(1, chips, finish, 0)

    def finish_kv(chip, _):
        for d in range(1, grp):
            send_kv(chip, d).wait_send()
        return 0

    lax.fori_loop(0, chips, finish_kv, 0)


def per_device(tokens, query_weight, key_value_weight, block_places, sinks):
    sp = lax.axis_size("sp")
    grp = lax.axis_size("grp")
    rows, width = tokens.shape
    group_rows = rows * sp
    key_count = grp * group_rows
    qc = query_weight.shape[1]
    qheads = qc // HEAD_SIZE
    kv_total = key_value_weight.shape[1] // (2 * HEAD_SIZE)
    freq = jnp.arange(HEAD_SIZE // 2, dtype=jnp.float32)
    inverse = rope_base ** (-(freq * 2.0) / HEAD_SIZE)
    inverse = jnp.tile(inverse, LANES // (HEAD_SIZE // 2)).reshape(1, LANES)

    vmem = pl.BlockSpec(memory_space=pltpu.VMEM)
    hbm = pl.BlockSpec(memory_space=pl.ANY)
    smem = pl.BlockSpec(memory_space=pltpu.SMEM)
    dma = pltpu.SemaphoreType.DMA
    return pl.pallas_call(
        functools.partial(kernel, grp, sp, qheads, kv_total),
        out_shape=jax.ShapeDtypeStruct((rows, qc * sp), jnp.bfloat16),
        in_specs=[vmem, hbm, hbm, vmem, smem, smem],
        out_specs=vmem,
        scratch_shapes=[
            pltpu.VMEM((sp, rows, width), jnp.bfloat16),
            pltpu.VMEM((width, qc), jnp.bfloat16),
            pltpu.VMEM((width, 2 * LANES), jnp.bfloat16),
            pltpu.VMEM((key_count, LANES), jnp.bfloat16),
            pltpu.VMEM((qheads, group_rows, LANES), jnp.bfloat16),
            pltpu.VMEM((sp, rows, qc), jnp.bfloat16),
            pltpu.VMEM((sp, rows, qc), jnp.bfloat16),
            pltpu.VMEM((group_rows, LANES), jnp.float32),
            pltpu.VMEM((group_rows, LANES), jnp.float32),
            pltpu.VMEM((group_rows, 1), jnp.int32),
            pltpu.VMEM((1, key_count), jnp.int32),
            dma((3,)),
            dma((sp,)),
            dma((sp,)),
            dma((sp,)),
            dma((grp, sp // 2)),
            dma((grp, sp // 2)),
            dma((sp,)),
            dma((sp,)),
        ],
        compiler_params=pltpu.CompilerParams(
            has_side_effects=True, vmem_limit_bytes=60 * 1024 * 1024
        ),
    )(tokens, query_weight, key_value_weight, inverse, block_places, sinks)


def solution(mesh):
    in_specs = (P(("grp", "sp"), None), P(None, "sp"), P(), P(), P())
    out_specs = P(("grp", "sp"), None)
    return jax.shard_map(
        per_device, mesh=mesh, in_specs=in_specs, out_specs=out_specs, check_vma=False
    )
```
